32 devices in a mesh: layer: 4 (over y, core), col: 4 (over z), row: 2 (over x).
Axes of the slice: x: 2, y: 2, z: 4, core: 2. Of those that a mesh axis runs over, the one named last changes fastest.
Arguments:
- activations: bfloat16 [4, 768, 4096], P(None, ('layer', 'row'), 'col'), may hold values from -6 to 6
- out_grads: bfloat16 [4, 768, 11008], P(None, ('layer', 'col'), 'row'), may hold values from -0.02734375 to 0.02734375
- basis_in: bfloat16 [4, 4096, 4096], P('layer', 'col', 'row'), may hold values from -0.09375 to 0.09375
- basis_out: bfloat16 [4, 11008, 11008], P('layer', 'row', 'col'), may hold values from -0.0546875 to 0.0546875
- eigenvalues: float32 [4, 11008, 4096], P('layer', 'col', 'row'), may hold values from 0.01 to 10
- damping: float32 [4], P('layer'), may hold values from 0.05 to 0.5
- layer_order: int32 [4], replicated, may hold values from 0 to 3, each once
- query_ids: int32 [256], replicated, may hold values from 0 to 3, never falling along the last dimension, each value on 1 to 128 neighbouring positions
- train_ids: int32 [512], replicated, may hold values from 0 to 15, never falling along the last dimension, each value on 1 to 64 neighbouring positions
Outputs:
- scores: float32 [4, 16], replicated
The draws below stay inside these ranges and needn't reach their ends.
Inputs may be any that keep to these rules, and one draw needn't show every extreme that they name: `layer_order`: each slot's layer appears once. `query_ids`: never falling; every query example has 1 to 128 tokens. `train_ids`: never falling; every train example has 1 to 64 tokens.
All inputs are finite; a program needn't handle non-finite values.
Results may differ from the reference program's by a relative error of at most 0.02.
Values may be sent and summed in bfloat16 or wider, within the bound.
A program may use at most 192 MiB of HBM per device.

```python
import math
import jax
import jax.numpy as jnp
import numpy as np
from jax import lax

DIN = 4096
DOUT = 11008
LAYERS = 4
QUERIES = 4
TRAIN = 16
QLEN = 64
TLEN = 32
QTOK = 256
TTOK = 512
QMOST = 128
TMOST = 64
N_COL = 4
N_ROW = 2


def level_of(stream_key, shape, cuts, least, top_value):
    gain = 1.0
    for position, parts in cuts:
        draws = jax.random.uniform(jax.random.fold_in(jax.random.fold_in(stream_key, 6), position), (parts,), jnp.float32, least / len(cuts), top_value / len(cuts))
        gain = gain * jnp.repeat(jnp.exp(draws), shape[position] // parts).reshape((-1,) + (1,) * (len(shape) - 1 - position))
    return gain


def length_profile(number_of, total, bound, lean):
    weights = [(1 << 20) // math.isqrt(standing ** lean) + 1 for standing in range(2, number_of + 1)]
    rest, holding = total - bound - (number_of - 1), [1] * (number_of - 1)
    while rest > 0:
        free = [i for i in range(number_of - 1) if holding[i] < bound]
        mass, remaining = sum([weights[i] for i in free]), rest
        for i in free:
            addition = min(bound - holding[i], max(1, remaining * weights[i] // mass), rest)
            holding[i] = holding[i] + addition
            rest = rest - addition
    return np.array([bound] + holding)


def ragged_sizes(rng, amount, total, most, skew):
    if amount == 2:
        one = jax.random.randint(rng, (), max(1, total - most), min(most, total - 1) + 1)
        return jnp.stack([one, total - one])
    lengths = jnp.asarray(length_profile(amount, total, most, skew), jnp.int32)
    twos = (amount - 1) // 2
    giver, receiver = lengths[1:1 + 2 * twos:2], lengths[2:2 + 2 * twos:2]
    room = jnp.minimum(giver - 1, most - receiver)
    moved = jax.random.randint(jax.random.fold_in(rng, 1), (twos,), 0, 1 << 20) % (room + 1)
    lengths = lengths.at[1:1 + 2 * twos:2].set(giver - moved).at[2:2 + 2 * twos:2].set(receiver + moved)
    return lengths[jax.random.permutation(jax.random.fold_in(rng, 2), amount)]


def normal_values(stream_key, extent, spread, reach, pieces=(), kind=jnp.bfloat16):
    array = spread * jax.random.normal(stream_key, extent, jnp.float32)
    if pieces:
        array = array * level_of(stream_key, extent, pieces, -0.22, 0.18)
    return jnp.clip(array, -reach, reach).astype(kind)


def setup_inputs(seed: int = 0) -> dict:
    streams_of = jax.random.split(jax.random.key(seed), 10)
    activations = normal_values(streams_of[0], (LAYERS, QTOK + TTOK, DIN), 1.0, 6.0, ((1, 8), (2, 4)))
    out_grads = normal_values(streams_of[1], (LAYERS, QTOK + TTOK, DOUT), ((QLEN * TLEN * DIN * DOUT) ** -0.25), 0.02734375, ((1, 16), (2, 2)))
    basis_in = normal_values(streams_of[2], (LAYERS, DIN, DIN), DIN ** -0.5, 0.09375, ((0, 4), (1, 4), (2, 2)))
    basis_out = normal_values(streams_of[3], (LAYERS, DOUT, DOUT), DOUT ** -0.5, 0.0546875, ((0, 4), (1, 2), (2, 4)))
    eigenvalues = jnp.clip(jnp.exp(math.log(10.0) - 6.9077553 * jax.random.uniform(streams_of[4], (LAYERS, DOUT, DIN), jnp.float32) ** level_of(streams_of[4], (LAYERS, DOUT, DIN), ((0, 4), (1, 4), (2, 2)), -0.2, 0.2)), 0.01, 10.0)
    damping = jnp.clip(jnp.exp(math.log(0.5) - 2.3025851 * jax.random.uniform(streams_of[5], (LAYERS,), jnp.float32) ** level_of(streams_of[5], (LAYERS,), ((0, 4),), -0.2, 0.2)), 0.05, 0.5)
    layer_order = jax.random.permutation(streams_of[6], LAYERS).astype(jnp.int32)
    query_ids = jnp.searchsorted(jnp.cumsum(ragged_sizes(streams_of[7], QUERIES, QTOK, QMOST, 1)), jnp.arange(QTOK), side="right").astype(jnp.int32)
    train_ids = jnp.searchsorted(jnp.cumsum(ragged_sizes(streams_of[8], TRAIN, TTOK, TMOST, 1)), jnp.arange(TTOK), side="right").astype(jnp.int32)
    return {"activations": activations, "out_grads": out_grads, "basis_in": basis_in, "basis_out": basis_out, "eigenvalues": eigenvalues, "damping": damping, "layer_order": layer_order, "query_ids": query_ids, "train_ids": train_ids}


def rotate(values, basis, blocks):
    width = basis.shape[0] // blocks
    total = jnp.zeros((values.shape[0], basis.shape[1]), jnp.float32)
    for index in range(blocks):
        piece = jnp.dot(values[:, index * width:(index + 1) * width], basis[index * width:(index + 1) * width], preferred_element_type=jnp.float32)
        rounded = lax.optimization_barrier(piece.astype(jnp.bfloat16))
        total = total + rounded.astype(jnp.float32)
    return total.astype(jnp.bfloat16)


def reference(activations, out_grads, basis_in, basis_out, eigenvalues, damping, layer_order, query_ids, train_ids):
    query_tokens = query_ids.shape[0]
    train_onehot = (train_ids[:, None] == jnp.arange(TRAIN, dtype=jnp.int32)[None, :]).astype(jnp.float32)
    total = jnp.zeros((QUERIES, TRAIN), jnp.float32)
    for slot in range(LAYERS):
        layer = layer_order[slot].astype(jnp.int32)
        inputs = lax.dynamic_index_in_dim(activations, layer, 0, keepdims=False)
        grads = lax.dynamic_index_in_dim(out_grads, layer, 0, keepdims=False)
        rotated_in = rotate(inputs, basis_in[slot], N_COL)
        rotated_out = rotate(grads, basis_out[slot], N_ROW)
        query_in = rotated_in[:query_tokens]
        query_out = rotated_out[:query_tokens]
        train_in = rotated_in[query_tokens:]
        train_out = rotated_out[query_tokens:]
        denominator = eigenvalues[slot] + damping[slot]

        def one_query(index):
            mask = (query_ids == index).astype(jnp.bfloat16)
            masked = query_in * mask[:, None]
            gram = jnp.dot(query_out.T, masked, preferred_element_type=jnp.float32)
            precond = (gram / denominator).astype(jnp.bfloat16)
            mapped = jnp.dot(train_out, precond, preferred_element_type=jnp.float32)
            return jnp.sum(mapped * train_in.astype(jnp.float32), axis=1)

        values = lax.map(one_query, jnp.arange(QUERIES, dtype=jnp.int32))
        total = total + jnp.dot(values, train_onehot, precision=lax.Precision.HIGHEST)
    return total
```

```python
import functools

import jax
import jax.numpy as jnp
from jax import lax
from jax.experimental import pallas as pl
from jax.experimental.pallas import tpu as pltpu
from jax.sharding import PartitionSpec as P

QUERIES = 4
TRAIN = 16
MESH = pl.DeviceIdType.MESH
VMEM_LIMIT = 66_000_000


def pairs_of(layer, layers):
    partner = layer + 1 - 2 * (layer % 2)
    return [layer, partner, (layer + 2) % layers, (partner + 2) % layers]


def gather_kernel(
    xa_hbm, xo_hbm, win_hbm, wout_hbm, a_out, b_out,
    w, xbuf, prcv, xa, term, rs,
    local_sem, xa_send, xa_recv, xy_send, x_recv, up_send, dn_send, p_send, p_recv,
    rs_send, rs_recv, ag_send, ag_recv,
):
    layers, cols, rows = lax.axis_size("layer"), lax.axis_size("col"), lax.axis_size("row")
    l, c, r = lax.axis_index("layer"), lax.axis_index("col"), lax.axis_index("row")
    order = pairs_of(l, layers)
    din, width_in = win_hbm.shape
    width = wout_hbm.shape[0]
    block = xbuf.shape[1]
    units = layers * cols
    last = cols - 1
    half = term.shape[1]

    def unit(layer, col):
        return col * layers + layer

    def order_at(j):
        return jnp.where(j == 0, order[0], jnp.where(j == 1, order[1], jnp.where(j == 2, order[2], order[3])))

    def remote(src, dst, send, recv, device):
        return pltpu.make_async_remote_copy(
            src_ref=src, dst_ref=dst, send_sem=send, recv_sem=recv, device_id=device, device_id_type=MESH
        )

    own = unit(l, c)
    own_copy = pltpu.make_async_copy(xo_hbm.at[l], xbuf.at[own], local_sem.at[0])
    own_copy.start()
    win_copy = pltpu.make_async_copy(win_hbm, w.at[pl.ds(0, din), pl.ds(0, width_in)], local_sem.at[1])
    win_copy.start()
    me_a = l * rows + r
    xa_copy = pltpu.make_async_copy(xa_hbm.at[l], xa.at[me_a], local_sem.at[2])
    xa_copy.start()

    def xa_remote(dl, dr):
        tl, tr = (l + dl) % layers, (r + dr) % rows
        return remote(
            xa_hbm.at[tl], xa.at[me_a], xa_send.at[dl * rows + dr], xa_recv.at[me_a], {"layer": tl, "row": tr}
        )

    offsets = [(dl, dr) for dl in (2, 3, 1, 0) for dr in range(rows) if (dl, dr) != (0, 0)]

    def xy_remote(j):
        return remote(
            xo_hbm.at[order[j]], xbuf.at[own], xy_send.at[j], x_recv.at[own], {"layer": order[j]}
        )

    def up(u):
        return remote(xbuf.at[u], xbuf.at[u], up_send.at[u], x_recv.at[u], {"col": c + 1})

    def down(u):
        return remote(xbuf.at[u], xbuf.at[u], dn_send.at[u], x_recv.at[u], {"col": c - 1})

    def wait_unit(u):
        remote(xbuf.at[u], xbuf.at[u], up_send.at[u], x_recv.at[u], {"col": c}).wait_recv()

    def send_own(j):
        u = unit(order[j], c)

        @pl.when(c < last)
        def _():
            up(u).start()

        @pl.when(c > 0)
        def _():
            down(u).start()

    xy_remote(1).start()
    for dl, dr in offsets:
        xa_remote(dl, dr).start()
    xy_remote(2).start()
    xy_remote(3).start()
    own_copy.wait()
    send_own(0)
    wait_unit(unit(order[1], c))
    send_own(1)

    win_copy.wait()
    xa_copy.wait()
    for dl, dr in offsets:
        src = ((l + dl) % layers) * rows + (r + dr) % rows
        remote(xa.at[src], xa.at[src], xa_send.at[0], xa_recv.at[src], {"layer": l}).wait_recv()

    step_in = 256
    tokens = xa.shape[0] * xa.shape[1]

    @pl.loop(0, width_in // step_in)
    def _(k):
        at = pl.ds(pl.multiple_of(k * step_in, step_in), step_in)
        part = jnp.dot(
            xa[...].reshape(tokens, din), w[pl.ds(0, din), at], preferred_element_type=jnp.float32
        ).astype(jnp.bfloat16)
        term[:, :, at] = part.reshape(term.shape[0], half, step_in)

    wout_copy = pltpu.make_async_copy(wout_hbm, w, local_sem.at[3])
    wout_copy.start()

    low, high = cols // 2 - 1, cols // 2
    owners = [low, high]

    def rs_remote(h, src):
        slot = src if src < owners[h] else src - 1
        return remote(term.at[h], rs.at[slot], rs_send.at[h], rs_recv.at[slot], {"col": owners[h]})

    for s in range(cols):
        @pl.when(c == s)
        def _(s=s):
            for h in (range(2) if s < high else reversed(range(2))):
                if owners[h] != s:
                    rs_remote(h, s).start()

    for j in (2, 3):
        wait_unit(unit(order[j], c))
        send_own(j)

    wout_copy.wait()

    tile = 256
    full = width // tile
    rest = width - full * tile

    def p_remote(u):
        return remote(b_out.at[u], prcv.at[u], p_send.at[u], p_recv.at[u], {"row": (r + 1) % rows})

    def rotate(layer, col):
        even = layer // 2 * 2

        def columns(at):
            part = lax.dot_general(
                xbuf[pl.ds(unit(even, col), 2)].reshape(2 * block, xbuf.shape[2]),
                w[at, :],
                (((1,), (1,)), ((), ())),
                preferred_element_type=jnp.float32,
            ).astype(jnp.bfloat16)
            b_out[even * cols + col, :, at] = part[:block]
            b_out[(even + 1) * cols + col, :, at] = part[block:]

        @pl.loop(0, full)
        def _(k):
            columns(pl.ds(pl.multiple_of(k * tile, tile), tile))

        if rest:
            columns(pl.ds(full * tile, rest))
        p_remote(even * cols + col).start()
        p_remote((even + 1) * cols + col).start()

    per = layers

    def step(m, with_own):
        hop = m // 2 + 1
        if with_own:
            rotate(order_at(m % 2 * 2), c)

        @pl.loop(0, 2)
        def _(k):
            lj = order_at(m % 2 * 2 + k)
            u_up, u_dn = unit(lj, c - hop), unit(lj, c + hop)

            @pl.when(c - hop >= 0)
            def _():
                wait_unit(u_up)

                @pl.when(c < last)
                def _():
                    up(u_up).start()

            @pl.when(c + hop <= last)
            def _():
                wait_unit(u_dn)

                @pl.when(c > 0)
                def _():
                    down(u_dn).start()

        @pl.loop(0, 2)
        def _(d):
            far = jnp.where(d == 0, c - hop, c + hop)

            @pl.when((far >= 0) & (far <= last))
            def _():
                rotate(order_at(m % 2 * 2), far)

    steps = 2 * last

    @pl.loop(0, steps - 2)
    def _(m):
        step(m, False)

    def ag_remote(h, way):
        return remote(
            a_out.at[h], a_out.at[h], ag_send.at[h, 0 if way > 0 else 1], ag_recv.at[h], {"col": c + way}
        )

    for h in range(2):
        @pl.when(c == owners[h])
        def _(h=h):
            for slot in range(cols - 1):
                remote(rs.at[slot], rs.at[slot], rs_send.at[h], rs_recv.at[slot], {"col": c}).wait_recv()

            chunk = 16

            @pl.loop(0, half // chunk)
            def _(k):
                at = pl.ds(pl.multiple_of(k * chunk, chunk), chunk)
                parts = [rs[s, at, :] for s in range(cols - 1)]
                parts.insert(owners[h], term[h, at, :])
                total = parts[0].astype(jnp.float32)
                for p in parts[1:]:
                    total = total + p.astype(jnp.float32)
                a_out[h, at, :] = total.astype(jnp.bfloat16)

            ag_remote(h, 1).start()
            ag_remote(h, -1).start()

    def ag_wait(h):
        remote(a_out.at[h], a_out.at[h], ag_send.at[h, 0], ag_recv.at[h], {"col": c}).wait_recv()

    step(steps - 2, True)

    @pl.when(c == high)
    def _():
        ag_wait(0)
        ag_remote(0, 1).start()

    @pl.when(c == low)
    def _():
        ag_wait(1)
        ag_remote(1, -1).start()

    step(steps - 1, True)

    @pl.loop(0, units)
    def _(u):
        p_remote(u).wait()
        b_out[u] = (b_out[u].astype(jnp.float32) + prcv[u].astype(jnp.float32)).astype(jnp.bfloat16)

    @pl.when((c < low) | (c > high))
    def _():
        ag_wait(0)
        ag_wait(1)

    for dl, dr in offsets:
        xa_remote(dl, dr).wait_send()
    for j in (1, 2, 3):
        xy_remote(j).wait_send()

    @pl.loop(0, units)
    def _(u):
        col = u // layers

        @pl.when((c < last) & (col <= c))
        def _():
            up(u).wait_send()

        @pl.when((c > 0) & (col >= c))
        def _():
            down(u).wait_send()

    for s in range(cols):
        @pl.when(c == s)
        def _(s=s):
            for h in range(2):
                if owners[h] != s:
                    rs_remote(h, s).wait_send()

    @pl.when(c == low)
    def _():
        ag_remote(0, 1).wait_send()
        ag_remote(0, -1).wait_send()
        ag_remote(1, -1).wait_send()

    @pl.when(c == high)
    def _():
        ag_remote(1, 1).wait_send()
        ag_remote(1, -1).wait_send()
        ag_remote(0, 1).wait_send()


def gathered(xa, xo, basis_in, basis_out, cols, rows):
    layers, block_in, din = xa.shape
    block = xo.shape[1]
    width_in, (width, dout) = basis_in.shape[1], basis_out.shape
    tokens = layers * cols * block
    units = layers * cols
    bf = jnp.bfloat16
    a, b = pl.pallas_call(
        gather_kernel,
        out_shape=(
            jax.ShapeDtypeStruct((2, tokens // 2, width_in), bf),
            jax.ShapeDtypeStruct((units, block, width), bf),
        ),
        in_specs=[pl.BlockSpec(memory_space=pltpu.HBM)] * 4,
        out_specs=(pl.BlockSpec(memory_space=pltpu.VMEM),) * 2,
        scratch_shapes=[
            pltpu.VMEM((width, dout), bf),
            pltpu.VMEM((units, block, dout), bf),
            pltpu.VMEM((units, block, width), bf),
            pltpu.VMEM((layers * rows, block_in, din), bf),
            pltpu.VMEM((2, tokens // 2, width_in), bf),
            pltpu.VMEM((cols - 1, tokens // 2, width_in), bf),
            pltpu.SemaphoreType.DMA((4,)),
            pltpu.SemaphoreType.DMA((layers * rows,)),
            pltpu.SemaphoreType.DMA((layers * rows,)),
            pltpu.SemaphoreType.DMA((layers,)),
            pltpu.SemaphoreType.DMA((units,)),
            pltpu.SemaphoreType.DMA((units,)),
            pltpu.SemaphoreType.DMA((units,)),
            pltpu.SemaphoreType.DMA((units,)),
            pltpu.SemaphoreType.DMA((units,)),
            pltpu.SemaphoreType.DMA((2,)),
            pltpu.SemaphoreType.DMA((cols - 1,)),
            pltpu.SemaphoreType.DMA((2, 2)),
            pltpu.SemaphoreType.DMA((2,)),
        ],
        compiler_params=pltpu.CompilerParams(has_side_effects=True, vmem_limit_bytes=VMEM_LIMIT),
        name="gather_rotate",
    )(xa, xo, basis_in, basis_out)
    return a.reshape(tokens, width_in), b.reshape(tokens, width)


def score_kernel(
    ids_ref, train_ref, damp_ref, eig_ref, a_ref, b_ref, out_ref,
    rinv, hbuf, acc, mine, parts, send_sem, recv_sem,
):
    j, last = pl.program_id(0), pl.num_programs(0) - 1
    sizes = [lax.axis_size(n) for n in ("layer", "col", "row")]
    l, c, r = [lax.axis_index(n) for n in ("layer", "col", "row")]
    devices = sizes[0] * sizes[1] * sizes[2]
    me = (l * sizes[1] + c) * sizes[2] + r
    barrier = pltpu.get_barrier_semaphore()

    def place(index):
        return {
            "layer": index // (sizes[1] * sizes[2]),
            "col": index // sizes[2] % sizes[1],
            "row": index % sizes[2],
        }

    @pl.when(j == 0)
    def _():
        @pl.loop(1, devices)
        def _(k):
            pl.semaphore_signal(barrier, inc=1, device_id=place((me + k) % devices), device_id_type=MESH)

        acc[...] = jnp.zeros_like(acc)

    queries = ids_ref.shape[0]
    rinv[...] = 1.0 / (eig_ref[...] + damp_ref[0])
    count, train, lanes = acc.shape
    for q in range(count):
        mask = (ids_ref[...] == q).astype(jnp.float32).astype(jnp.bfloat16)
        masked = a_ref[:queries, :] * mask
        gram = lax.dot_general(
            b_ref[:queries, :], masked, (((0,), (0,)), ((), ())), preferred_element_type=jnp.float32
        )
        hbuf[...] = (gram * rinv[...]).astype(jnp.bfloat16)
        mapped = jnp.dot(b_ref[queries:, :], hbuf[...], preferred_element_type=jnp.float32)
        value = mapped * a_ref[queries:, :].astype(jnp.float32)
        total = value[:, :lanes]
        for k in range(1, value.shape[1] // lanes):
            total = total + value[:, k * lanes : (k + 1) * lanes]
        acc[q] += total

    def remote(k, target):
        return pltpu.make_async_remote_copy(
            src_ref=mine, dst_ref=parts.at[me], send_sem=send_sem.at[k], recv_sem=recv_sem.at[me],
            device_id=place(target), device_id_type=MESH,
        )

    @pl.when(j == last)
    def _():
        ids = lax.broadcasted_iota(jnp.int32, (lanes, train), 0)
        onehot = (ids == train_ref[...]).astype(jnp.float32)
        row = lax.broadcasted_iota(jnp.int32, mine.shape, 0)
        ones = jnp.ones((mine.shape[0], lanes), jnp.float32)
        dims = (((1,), (1,)), ((), ()))
        total = jnp.zeros(mine.shape, jnp.float32)
        for q in range(count):
            value = lax.dot_general(ones, acc[q], dims, precision=lax.Precision.HIGHEST,
                                    preferred_element_type=jnp.float32)
            score = lax.dot_general(value, onehot, dims, precision=lax.Precision.HIGHEST,
                                    preferred_element_type=jnp.float32)
            total = total + jnp.where(row == q, score, 0.0)
        mine[...] = total
        pl.semaphore_wait(barrier, devices - 1)

        @pl.loop(1, devices)
        def _(k):
            remote(k, (me + k) % devices).start()

        parts[me] = mine[...]

        @pl.loop(1, devices)
        def _(k):
            source = (me + k) % devices
            pltpu.make_async_remote_copy(
                src_ref=mine, dst_ref=parts.at[source], send_sem=send_sem.at[k], recv_sem=recv_sem.at[source],
                device_id=place(source), device_id_type=MESH,
            ).wait()

        full = parts[0]
        for k in range(1, devices):
            full = full + parts[k]
        out_ref[...] = full


def scored(a, b, eig, damping, query_ids, train_ids):
    tokens, width_in = a.shape
    width = b.shape[1]
    queries, train = query_ids.shape[0], train_ids.shape[0]
    tile, lanes, held = 256, 128, 8
    devices = lax.axis_size("layer") * lax.axis_size("col") * lax.axis_size("row")
    bf, f32 = jnp.bfloat16, jnp.float32
    out = pl.pallas_call(
        score_kernel,
        out_shape=jax.ShapeDtypeStruct((held, lanes), f32),
        grid=(width_in // tile,),
        in_specs=[
            pl.BlockSpec((queries, 1), lambda j: (0, 0)),
            pl.BlockSpec((1, train), lambda j: (0, 0)),
            pl.BlockSpec(memory_space=pltpu.SMEM),
            pl.BlockSpec((width, tile), lambda j: (0, j)),
            pl.BlockSpec((tokens, tile), lambda j: (0, j)),
            pl.BlockSpec((tokens, width), lambda j: (0, 0)),
        ],
        out_specs=pl.BlockSpec((held, lanes), lambda j: (0, 0)),
        scratch_shapes=[
            pltpu.VMEM((width, tile), f32),
            pltpu.VMEM((width, tile), bf),
            pltpu.VMEM((QUERIES, train, lanes), f32),
            pltpu.VMEM((held, lanes), f32),
            pltpu.VMEM((devices, held, lanes), f32),
            pltpu.SemaphoreType.DMA((devices,)),
            pltpu.SemaphoreType.DMA((devices,)),
        ],
        compiler_params=pltpu.CompilerParams(
            dimension_semantics=("arbitrary",), vmem_limit_bytes=VMEM_LIMIT,
            has_side_effects=True, collective_id=1,
        ),
        name="precond_scores",
    )(query_ids[:, None], train_ids[None, :], damping, eig, a, b)
    return out[:QUERIES, :TRAIN]


def fast_body(
    activations, out_grads, basis_in, basis_out, eigenvalues, damping, layer_order, query_ids, train_ids
):
    cols, rows = lax.axis_size("col"), lax.axis_size("row")
    xa = activations.at[layer_order].get(mode="promise_in_bounds")
    xo = out_grads.at[layer_order].get(mode="promise_in_bounds")
    a, b = gathered(xa, xo, basis_in[0], basis_out[0].T, cols, rows)
    return scored(a, b, eigenvalues[0], damping, query_ids, train_ids)


def ring_pieces(blocks, col_count):
    up = [(s, (s + 1) % col_count) for s in range(col_count)]
    down = [(s, (s - 1) % col_count) for s in range(col_count)]
    steps = [blocks]
    for _ in range(col_count - 1):
        steps.append(
            [lax.ppermute(b, "col", down if i % 2 else up) for i, b in enumerate(steps[-1])]
        )
    return steps


def row_sum(term, row_count):
    if row_count == 2:
        other = lax.ppermute(term, "row", [(0, 1), (1, 0)])
        return (term.astype(jnp.float32) + other.astype(jnp.float32)).astype(jnp.bfloat16)
    return lax.psum(term, "row")


def body(
    activations,
    out_grads,
    basis_in,
    basis_out,
    eigenvalues,
    damping,
    layer_order,
    query_ids,
    train_ids,
):
    layer_groups = lax.axis_size("layer")
    row_count = lax.axis_size("row")
    col_count = lax.axis_size("col")
    me = lax.axis_index("col")
    query_tokens = query_ids.shape[0]

    ordered_in = jnp.take(activations, layer_order, axis=0)
    in_block = ordered_in.shape[1]
    moved_in = lax.all_to_all(ordered_in, "layer", split_axis=0, concat_axis=1, tiled=True)
    shaped_in = moved_in.reshape(layer_groups, in_block, moved_in.shape[2])
    joined_in = lax.all_gather(shaped_in, "row", axis=1, tiled=True)
    inputs_full = joined_in.reshape(layer_groups * row_count * in_block, moved_in.shape[2])
    partial_in = jnp.dot(inputs_full, basis_in[0], preferred_element_type=jnp.float32)
    rotated_in = lax.psum(partial_in.astype(jnp.bfloat16), "col")

    ordered_out = jnp.take(out_grads, layer_order, axis=0)
    block = ordered_out.shape[1]
    moved_out = lax.all_to_all(ordered_out, "layer", split_axis=0, concat_axis=1, tiled=True)
    moved_out = moved_out.reshape(layer_groups, block, moved_out.shape[2])

    def rotate(pieces):
        tokens = jnp.concatenate(pieces, axis=0)
        partial = jnp.dot(tokens, basis_out[0], preferred_element_type=jnp.float32)
        return row_sum(partial.astype(jnp.bfloat16), row_count)

    head = min(layer_groups, -(-query_tokens // (col_count * block)))
    first = ring_pieces([moved_out[l] for l in range(head)], col_count)
    second = ring_pieces([moved_out[l] for l in range(head, layer_groups)], col_count)

    def source(step, i):
        return lax.rem(me + (step if i % 2 else col_count - step), col_count)

    width = basis_out.shape[2]
    front = jnp.zeros((head, col_count, block, width), jnp.bfloat16)
    for begin in range(0, col_count, 2):
        steps = range(begin, min(begin + 2, col_count))
        rotated = rotate([b for s in steps for b in first[s]])
        rotated = rotated.reshape(len(steps), head, 1, block, width)
        for n, s in enumerate(steps):
            for i in range(head):
                front = lax.dynamic_update_slice(
                    front, rotated[n, i][None], (i, source(s, i), 0, 0)
                )
    front = front.reshape(head * col_count * block, width)

    query_mask = (query_ids[None, :] == jnp.arange(QUERIES, dtype=jnp.int32)[:, None]).astype(
        jnp.bfloat16
    )
    query_in = rotated_in[:query_tokens]
    query_out = front[:query_tokens]
    masked = query_mask[:, :, None] * query_in[None, :, :]
    query_gram = jnp.einsum("si,qsj->qij", query_out, masked, preferred_element_type=jnp.float32)
    precond = (query_gram / (eigenvalues[0] + damping[0])).astype(jnp.bfloat16)

    def scores_of(train_out, train_in, ids):
        onehot = (ids[:, None] == jnp.arange(TRAIN, dtype=jnp.int32)[None, :]).astype(jnp.float32)
        mapped = jnp.einsum("ui,qij->quj", train_out, precond, preferred_element_type=jnp.float32)
        values = jnp.sum(mapped * train_in[None, :, :], axis=2)
        return jnp.dot(values, onehot, precision=lax.Precision.HIGHEST)

    front_tokens = head * col_count * block
    total = jnp.zeros((QUERIES, TRAIN), jnp.float32)
    if front_tokens > query_tokens:
        total = total + scores_of(
            front[query_tokens:],
            rotated_in[query_tokens:front_tokens],
            train_ids[: front_tokens - query_tokens],
        )

    if head < layer_groups:
        groups = [list(range(b, min(b + 2, col_count))) for b in range(0, col_count, 2)]
        if len(groups[-1]) == 2:
            groups[-1:] = [[groups[-1][0]], [groups[-1][1]]]
        for steps in groups:
            train_out = rotate([b for s in steps for b in second[s]])
            train_in, ids = [], []
            for s in steps:
                for i in range(layer_groups - head):
                    start = ((head + i) * col_count + source(s, i)) * block
                    train_in.append(lax.dynamic_slice_in_dim(rotated_in, start, block, 0))
                    ids.append(lax.dynamic_slice_in_dim(train_ids, start - query_tokens, block, 0))
            total = total + scores_of(
                train_out, jnp.concatenate(train_in, axis=0), jnp.concatenate(ids, axis=0)
            )
    return lax.psum(total, ("layer", "col", "row"))


def solution(mesh):
    in_specs = (
        P(None, ("layer", "row"), "col"),
        P(None, ("layer", "col"), "row"),
        P("layer", "col", "row"),
        P("layer", "row", "col"),
        P("layer", "col", "row"),
        P("layer"),
        P(),
        P(),
        P(),
    )
    out_specs = P()
    sizes = [mesh.shape[n] for n in ("layer", "col", "row")]
    run = fast_body if sizes == [4, 4, 2] else body
    return jax.shard_map(run, mesh=mesh, in_specs=in_specs, out_specs=out_specs, check_vma=False)
```

```python
import functools

import jax
import jax.numpy as jnp
from jax import lax
from jax.experimental import pallas as pl
from jax.experimental.pallas import tpu as pltpu
from jax.sharding import PartitionSpec as P

QUERIES = 4
TRAIN = 16
MESH = pl.DeviceIdType.MESH
VMEM_LIMIT = 67_043_328


def pairs_of(layer, layers):
    partner = layer + 1 - 2 * (layer % 2)
    return [layer, partner, (layer + 2) % layers, (partner + 2) % layers]


def score_kernel(
    xa_hbm, xo_hbm, win_hbm, wout_hbm, eig_hbm, damp_ref, ids_ref, train_ref, out_ref,
    w, xbuf, prcv, xa, term, rs, a_full, b_full, eig, acc, mine, parts,
    local_sem, xa_send, xa_recv, xy_send, x_recv, in_send, ex_send, p_send, p_recv,
    rs_send, rs_recv, ag_send, ag_recv, eig_sem, sum_send, sum_recv,
):
    layers, cols, rows = lax.axis_size("layer"), lax.axis_size("col"), lax.axis_size("row")
    l, c, r = lax.axis_index("layer"), lax.axis_index("col"), lax.axis_index("row")
    order = pairs_of(l, layers)
    din, width_in = win_hbm.shape
    width = wout_hbm.shape[0]
    block = xbuf.shape[1]
    units = layers * cols
    last = cols - 1
    half = term.shape[1]
    side = c // (cols // 2)
    way = 1 - 2 * side
    inner = (c > 0) & (c < last)
    outer = (c == 0) | (c == last)

    def unit(layer, col):
        return col * layers + layer

    def remote(src, dst, send, recv, device):
        return pltpu.make_async_remote_copy(
            src_ref=src, dst_ref=dst, send_sem=send, recv_sem=recv, device_id=device, device_id_type=MESH
        )

    span = eig.shape[2]
    spans = width_in // span

    def eig_copy(k):
        at = pl.ds(pl.multiple_of(k * span, span), span)
        return pltpu.make_async_copy(eig_hbm.at[:, at], eig.at[k % 2], eig_sem.at[k % 2])

    own = unit(l, c)
    own_copy = pltpu.make_async_copy(xo_hbm.at[l], xbuf.at[own], local_sem.at[0])
    own_copy.start()
    win_copy = pltpu.make_async_copy(win_hbm, w.at[pl.ds(0, din), pl.ds(0, width_in)], local_sem.at[1])
    win_copy.start()
    me_a = l * rows + r
    xa_copy = pltpu.make_async_copy(xa_hbm.at[l], xa.at[me_a], local_sem.at[2])
    xa_copy.start()

    def xa_remote(dl, dr):
        tl, tr = (l + dl) % layers, (r + dr) % rows
        return remote(
            xa_hbm.at[tl], xa.at[me_a], xa_send.at[dl * rows + dr], xa_recv.at[me_a], {"layer": tl, "row": tr}
        )

    offsets = [(dl, dr) for dl in (2, 3, 1, 0) for dr in range(rows) if (dl, dr) != (0, 0)]

    def xy_remote(j):
        return remote(
            xo_hbm.at[order[j]], xbuf.at[own], xy_send.at[j], x_recv.at[own], {"layer": order[j]}
        )

    def inward(u):
        return remote(xbuf.at[u], xbuf.at[u], in_send.at[u], x_recv.at[u], {"col": c + way})

    def outward(u):
        return remote(xbuf.at[u], xbuf.at[u], ex_send.at[u], x_recv.at[u], {"col": c - way})

    def wait_unit(u):
        remote(xbuf.at[u], xbuf.at[u], in_send.at[u], x_recv.at[u], {"col": c}).wait_recv()

    def send_own(j):
        u = unit(order[j], c)
        inward(u).start()

        @pl.when(inner)
        def _():
            outward(u).start()

    xy_remote(1).start()
    for dl, dr in offsets:
        xa_remote(dl, dr).start()
    xy_remote(2).start()
    xy_remote(3).start()
    own_copy.wait()
    send_own(0)
    wait_unit(unit(order[1], c))
    send_own(1)

    win_copy.wait()
    xa_copy.wait()
    for dl, dr in offsets:
        src = ((l + dl) % layers) * rows + (r + dr) % rows
        remote(xa.at[src], xa.at[src], xa_send.at[0], xa_recv.at[src], {"layer": l}).wait_recv()

    step_in = 256
    tokens = xa.shape[0] * xa.shape[1]

    @pl.loop(0, width_in // step_in)
    def _(k):
        at = pl.ds(pl.multiple_of(k * step_in, step_in), step_in)
        part = jnp.dot(
            xa[...].reshape(tokens, din), w[pl.ds(0, din), at], preferred_element_type=jnp.float32
        ).astype(jnp.bfloat16)
        term[:, :, at] = part.reshape(term.shape[0], half, step_in)

    wout_copy = pltpu.make_async_copy(wout_hbm, w, local_sem.at[3])
    wout_copy.start()
    eig_copy(0).start()
    eig_copy(1).start()

    def rs_remote(h, slot):
        dst = rs.at[slot] if slot < 2 else a_full.at[h]
        return remote(term.at[h], dst, rs_send.at[slot], rs_recv.at[slot], {"col": c + way})

    def rs_wait(slot):
        dst = rs.at[slot] if slot < 2 else a_full.at[side]
        remote(dst, dst, rs_send.at[slot], rs_recv.at[slot], {"col": c}).wait_recv()

    @pl.when(outer)
    def _():
        rs_remote(1 - side, 0).start()

    for j in (2, 3):
        wait_unit(unit(order[j], c))
        send_own(j)

    @pl.when(outer)
    def _():
        rs_remote(side, 1).start()

    def far_side(hop, j):
        @pl.when(outer if hop == last else (c >= 0))
        def _():
            for k in (j, j + 1):
                u = unit(order[k], c + way * hop)
                wait_unit(u)

                @pl.when(inner)
                def _():
                    outward(u).start()

    def near_side(j):
        @pl.when(inner)
        def _():
            for k in (j, j + 1):
                u = unit(order[k], c - way)
                wait_unit(u)
                inward(u).start()

    tile = 256
    full = width // tile
    rest = width - full * tile

    def rows_of(u):
        return pl.ds(pl.multiple_of(u * block, block), block)

    def p_remote(u):
        return remote(b_full.at[rows_of(u)], prcv.at[u], p_send.at[u], p_recv.at[u], {"row": (r + 1) % rows})

    def rotate(col, j, valid=None):
        even, amount = (0, layers) if j is None else (order[j] // 2 * 2, 2)

        def columns(at):
            part = lax.dot_general(
                xbuf[pl.ds(unit(even, col), amount)].reshape(amount * block, xbuf.shape[2]),
                w[at, :],
                (((1,), (1,)), ((), ())),
                preferred_element_type=jnp.float32,
            ).astype(jnp.bfloat16)
            for i in range(amount):
                b_full[rows_of((even + i) * cols + col), at] = part[i * block : (i + 1) * block]

        def run():
            @pl.loop(0, full)
            def _(k):
                columns(pl.ds(pl.multiple_of(k * tile, tile), tile))

            if rest:
                columns(pl.ds(full * tile, rest))
            for i in range(amount):
                p_remote((even + i) * cols + col).start()

        if valid is None:
            run()
        else:
            pl.when(valid)(run)

    def add(h, others, dst):
        chunk = 16

        @pl.loop(0, half // chunk)
        def _(k):
            at = pl.ds(pl.multiple_of(k * chunk, chunk), chunk)
            total = term[h, at, :].astype(jnp.float32)
            for other, i in others:
                total = total + other[i, at, :].astype(jnp.float32)
            dst[h, at, :] = total.astype(jnp.bfloat16)

    def ag_remote(h, to, k):
        at = a_full.at[h, :, pl.ds(pl.multiple_of(k * span, span), span)]
        return remote(at, at, ag_send.at[h, (to + 1) // 2, k], ag_recv.at[h, k], {"col": c + way * to})

    def ag_wait(h, k):
        at = a_full.at[h, :, pl.ds(pl.multiple_of(k * span, span), span)]
        remote(at, at, ag_send.at[h, 0, k], ag_recv.at[h, k], {"col": c}).wait_recv()

    def pass_on(begin, end):
        @pl.when(inner)
        def _():
            @pl.loop(begin, end)
            def _(k):
                ag_remote(side, -1, k).start()
                ag_wait(1 - side, k)
                ag_remote(1 - side, -1, k).start()

    far_side(1, 0)
    near_side(0)
    far_side(1, 2)
    wout_copy.wait()
    rotate(c + way, None)

    @pl.when(inner)
    def _():
        rs_wait(0)
        add(1 - side, ((rs, 0),), term)
        rs_remote(1 - side, 2).start()

    far_side(2, 0)
    rotate(c, None)
    near_side(2)
    rotate(c + 2 * way, 0, inner)
    rotate(c - way, None, inner)

    @pl.when(inner)
    def _():
        rs_wait(1)
        rs_wait(2)
        add(side, ((rs, 1), (a_full, side)), a_full)

        @pl.loop(0, spans)
        def _(k):
            ag_remote(side, 1, k).start()

    far_side(2, 2)
    rotate(c + 2 * way, None, outer)
    pass_on(0, spans // 2)
    rotate(c + 2 * way, 2, inner)
    pass_on(spans // 2, spans)
    far_side(3, 0)
    rotate(c + 3 * way, 0, outer)
    far_side(3, 2)
    rotate(c + 3 * way, 2, outer)

    @pl.loop(0, units)
    def _(u):
        p_remote(u).wait()
        at = rows_of(u)
        b_full[at, :] = (b_full[at, :].astype(jnp.float32) + prcv[u].astype(jnp.float32)).astype(jnp.bfloat16)

    acc[...] = jnp.zeros_like(acc)
    count, train, lanes = acc.shape
    queries = ids_ref.shape[0]
    rest_rows = half - queries
    part = 5 * lanes
    cuts = [(b, min(part, width - b)) for b in range(0, width, part)]

    @pl.loop(0, spans)
    def _(k):
        @pl.when(outer)
        def _():
            ag_wait(side, k)
            ag_wait(1 - side, k)

        eig_copy(k).wait()
        slot = k % 2
        at = pl.ds(pl.multiple_of(k * span, span), span)
        for begin, size in cuts:
            cut = pl.ds(begin, size)
            eig[slot, cut, :] = 1.0 / (eig[slot, cut, :] + damp_ref[0])
        for q in range(count):
            mask = (ids_ref[...] == q).astype(jnp.float32).astype(jnp.bfloat16)
            masked = a_full[0, :queries, at] * mask
            for begin, size in cuts:
                cut = pl.ds(begin, size)
                gram = lax.dot_general(
                    b_full[:queries, cut], masked, (((0,), (0,)), ((), ())), preferred_element_type=jnp.float32
                )
                w[cut, pl.ds(q * span, span)] = (gram * eig[slot, cut, :]).astype(jnp.bfloat16)
            mapped = jnp.dot(
                b_full[queries:, :], w[:, pl.ds(q * span, span)], preferred_element_type=jnp.float32
            )

            def gather(lo, n, h, first):
                value = mapped[lo : lo + n] * a_full[h, pl.ds(first, n), at].astype(jnp.float32)
                total = value[:, :lanes]
                for i in range(1, span // lanes):
                    total = total + value[:, i * lanes : (i + 1) * lanes]
                acc[q, pl.ds(lo, n), :] += total

            gather(0, rest_rows, 0, queries)
            gather(rest_rows, half, 1, 0)

        @pl.when(k + 2 < spans)
        def _():
            eig_copy(k + 2).start()

    devices = layers * cols * rows
    me = (l * cols + c) * rows + r

    def place(index):
        return {"layer": index // (cols * rows), "col": index // rows % cols, "row": index % rows}

    ids = lax.broadcasted_iota(jnp.int32, (lanes, train), 0)
    onehot = (ids == train_ref[...]).astype(jnp.float32)
    row = lax.broadcasted_iota(jnp.int32, mine.shape, 0)
    ones = jnp.ones((mine.shape[0], lanes), jnp.float32)
    dims = (((1,), (1,)), ((), ()))
    total = jnp.zeros(mine.shape, jnp.float32)
    for q in range(count):
        value = lax.dot_general(ones, acc[q], dims, precision=lax.Precision.HIGHEST,
                                preferred_element_type=jnp.float32)
        score = lax.dot_general(value, onehot, dims, precision=lax.Precision.HIGHEST,
                                preferred_element_type=jnp.float32)
        total = total + jnp.where(row == q, score, 0.0)
    mine[...] = total

    @pl.loop(1, devices)
    def _(k):
        remote(mine, parts.at[me], sum_send.at[k], sum_recv.at[me], place((me + k) % devices)).start()

    parts[me] = mine[...]

    for dl, dr in offsets:
        xa_remote(dl, dr).wait_send()
    for j in (1, 2, 3):
        xy_remote(j).wait_send()
    for j in range(layers):
        inward(unit(order[j], c)).wait_send()

        @pl.when(inner)
        def _(j=j):
            outward(unit(order[j], c)).wait_send()
            inward(unit(order[j], c - way)).wait_send()
            outward(unit(order[j], c + way)).wait_send()
            outward(unit(order[j], c + 2 * way)).wait_send()

    @pl.when(outer)
    def _():
        rs_remote(1 - side, 0).wait_send()
        rs_remote(side, 1).wait_send()

    @pl.when(inner)
    def _():
        rs_remote(1 - side, 2).wait_send()

        @pl.loop(0, spans)
        def _(k):
            ag_remote(side, 1, k).wait_send()
            ag_remote(side, -1, k).wait_send()
            ag_remote(1 - side, -1, k).wait_send()

    @pl.loop(1, devices)
    def _(k):
        source = (me + k) % devices
        remote(mine, parts.at[source], sum_send.at[k], sum_recv.at[source], place(source)).wait()

    full_sum = parts[0]
    for k in range(1, devices):
        full_sum = full_sum + parts[k]
    out_ref[...] = full_sum


def fast_body(
    activations, out_grads, basis_in, basis_out, eigenvalues, damping, layer_order, query_ids, train_ids
):
    cols, rows = lax.axis_size("col"), lax.axis_size("row")
    xa = activations.at[layer_order].get(mode="promise_in_bounds")
    xo = out_grads.at[layer_order].get(mode="promise_in_bounds")
    basis_out = basis_out[0].T
    layers, block_in, din = xa.shape
    block = xo.shape[1]
    width_in, (width, dout) = basis_in.shape[2], basis_out.shape
    tokens = layers * cols * block
    units = layers * cols
    devices = units * rows
    span, lanes, held = 256, 128, 8
    spans = width_in // span
    bf, f32 = jnp.bfloat16, jnp.float32
    hbm, vmem = pl.BlockSpec(memory_space=pltpu.HBM), pl.BlockSpec(memory_space=pltpu.VMEM)
    counts = [
        (4,), (layers * rows,), (layers * rows,), (layers,), (units,), (units,), (units,), (units,), (units,),
        (3,), (3,), (2, 2, spans), (2, spans), (2,), (devices,), (devices,),
    ]
    out = pl.pallas_call(
        score_kernel,
        out_shape=jax.ShapeDtypeStruct((held, lanes), f32),
        in_specs=[hbm] * 5 + [pl.BlockSpec(memory_space=pltpu.SMEM), vmem, vmem],
        out_specs=vmem,
        scratch_shapes=[
            pltpu.VMEM((width, dout), bf),
            pltpu.VMEM((units, block, dout), bf),
            pltpu.VMEM((units, block, width), bf),
            pltpu.VMEM((layers * rows, block_in, din), bf),
            pltpu.VMEM((2, tokens // 2, width_in), bf),
            pltpu.VMEM((2, tokens // 2, width_in), bf),
            pltpu.VMEM((2, tokens // 2, width_in), bf),
            pltpu.VMEM((tokens, width), bf),
            pltpu.VMEM((2, width, span), f32),
            pltpu.VMEM((QUERIES, train_ids.shape[0], lanes), f32),
            pltpu.VMEM((held, lanes), f32),
            pltpu.VMEM((devices, held, lanes), f32),
        ] + [pltpu.SemaphoreType.DMA(n) for n in counts],
        compiler_params=pltpu.CompilerParams(has_side_effects=True, vmem_limit_bytes=VMEM_LIMIT),
        name="mega_scores",
    )(xa, xo, basis_in[0], basis_out, eigenvalues[0], damping, query_ids[:, None], train_ids[None, :])
    return out[:QUERIES, :TRAIN]


def ring_pieces(blocks, col_count):
    up = [(s, (s + 1) % col_count) for s in range(col_count)]
    down = [(s, (s - 1) % col_count) for s in range(col_count)]
    steps = [blocks]
    for _ in range(col_count - 1):
        steps.append(
            [lax.ppermute(b, "col", down if i % 2 else up) for i, b in enumerate(steps[-1])]
        )
    return steps


def row_sum(term, row_count):
    if row_count == 2:
        other = lax.ppermute(term, "row", [(0, 1), (1, 0)])
        return (term.astype(jnp.float32) + other.astype(jnp.float32)).astype(jnp.bfloat16)
    return lax.psum(term, "row")


def body(
    activations,
    out_grads,
    basis_in,
    basis_out,
    eigenvalues,
    damping,
    layer_order,
    query_ids,
    train_ids,
):
    layer_groups = lax.axis_size("layer")
    row_count = lax.axis_size("row")
    col_count = lax.axis_size("col")
    me = lax.axis_index("col")
    query_tokens = query_ids.shape[0]

    ordered_in = jnp.take(activations, layer_order, axis=0)
    in_block = ordered_in.shape[1]
    moved_in = lax.all_to_all(ordered_in, "layer", split_axis=0, concat_axis=1, tiled=True)
    shaped_in = moved_in.reshape(layer_groups, in_block, moved_in.shape[2])
    joined_in = lax.all_gather(shaped_in, "row", axis=1, tiled=True)
    inputs_full = joined_in.reshape(layer_groups * row_count * in_block, moved_in.shape[2])
    partial_in = jnp.dot(inputs_full, basis_in[0], preferred_element_type=jnp.float32)
    rotated_in = lax.psum(partial_in.astype(jnp.bfloat16), "col")

    ordered_out = jnp.take(out_grads, layer_order, axis=0)
    block = ordered_out.shape[1]
    moved_out = lax.all_to_all(ordered_out, "layer", split_axis=0, concat_axis=1, tiled=True)
    moved_out = moved_out.reshape(layer_groups, block, moved_out.shape[2])

    def rotate(pieces):
        tokens = jnp.concatenate(pieces, axis=0)
        partial = jnp.dot(tokens, basis_out[0], preferred_element_type=jnp.float32)
        return row_sum(partial.astype(jnp.bfloat16), row_count)

    head = min(layer_groups, -(-query_tokens // (col_count * block)))
    first = ring_pieces([moved_out[l] for l in range(head)], col_count)
    second = ring_pieces([moved_out[l] for l in range(head, layer_groups)], col_count)

    def source(step, i):
        return lax.rem(me + (step if i % 2 else col_count - step), col_count)

    width = basis_out.shape[2]
    front = jnp.zeros((head, col_count, block, width), jnp.bfloat16)
    for begin in range(0, col_count, 2):
        steps = range(begin, min(begin + 2, col_count))
        rotated = rotate([b for s in steps for b in first[s]])
        rotated = rotated.reshape(len(steps), head, 1, block, width)
        for n, s in enumerate(steps):
            for i in range(head):
                front = lax.dynamic_update_slice(
                    front, rotated[n, i][None], (i, source(s, i), 0, 0)
                )
    front = front.reshape(head * col_count * block, width)

    query_mask = (query_ids[None, :] == jnp.arange(QUERIES, dtype=jnp.int32)[:, None]).astype(
        jnp.bfloat16
    )
    query_in = rotated_in[:query_tokens]
    query_out = front[:query_tokens]
    masked = query_mask[:, :, None] * query_in[None, :, :]
    query_gram = jnp.einsum("si,qsj->qij", query_out, masked, preferred_element_type=jnp.float32)
    precond = (query_gram / (eigenvalues[0] + damping[0])).astype(jnp.bfloat16)

    def scores_of(train_out, train_in, ids):
        onehot = (ids[:, None] == jnp.arange(TRAIN, dtype=jnp.int32)[None, :]).astype(jnp.float32)
        mapped = jnp.einsum("ui,qij->quj", train_out, precond, preferred_element_type=jnp.float32)
        values = jnp.sum(mapped * train_in[None, :, :], axis=2)
        return jnp.dot(values, onehot, precision=lax.Precision.HIGHEST)

    front_tokens = head * col_count * block
    total = jnp.zeros((QUERIES, TRAIN), jnp.float32)
    if front_tokens > query_tokens:
        total = total + scores_of(
            front[query_tokens:],
            rotated_in[query_tokens:front_tokens],
            train_ids[: front_tokens - query_tokens],
        )

    if head < layer_groups:
        groups = [list(range(b, min(b + 2, col_count))) for b in range(0, col_count, 2)]
        if len(groups[-1]) == 2:
            groups[-1:] = [[groups[-1][0]], [groups[-1][1]]]
        for steps in groups:
            train_out = rotate([b for s in steps for b in second[s]])
            train_in, ids = [], []
            for s in steps:
                for i in range(layer_groups - head):
                    start = ((head + i) * col_count + source(s, i)) * block
                    train_in.append(lax.dynamic_slice_in_dim(rotated_in, start, block, 0))
                    ids.append(lax.dynamic_slice_in_dim(train_ids, start - query_tokens, block, 0))
            total = total + scores_of(
                train_out, jnp.concatenate(train_in, axis=0), jnp.concatenate(ids, axis=0)
            )
    return lax.psum(total, ("layer", "col", "row"))


def solution(mesh):
    in_specs = (
        P(None, ("layer", "row"), "col"),
        P(None, ("layer", "col"), "row"),
        P("layer", "col", "row"),
        P("layer", "row", "col"),
        P("layer", "col", "row"),
        P("layer"),
        P(),
        P(),
        P(),
    )
    out_specs = P()
    sizes = [mesh.shape[n] for n in ("layer", "col", "row")]
    run = fast_body if sizes == [4, 4, 2] else body
    return jax.shard_map(run, mesh=mesh, in_specs=in_specs, out_specs=out_specs, check_vma=False)
```
